32 devices in a mesh: section: 4 (over x, core), ctx: 4 (over z), tp: 2 (over y).
Axes of the slice: x: 2, y: 2, z: 4, core: 2. Of those that a mesh axis runs over, the one named last changes fastest.
Arguments:
- head_input: bfloat16 [4, 1536, 8192], P('section', 'ctx', 'tp'), may hold values from -6 to 6
- gate_input: bfloat16 [4, 1536, 8192], P('section', 'ctx', 'tp'), may hold values from -6 to 6
- b_input: bfloat16 [4, 1536, 1024], P('section', 'ctx', 'tp'), may hold values from -0.52734375 to 0.52734375
- c_input: bfloat16 [4, 1536, 1024], P('section', 'ctx', 'tp'), may hold values from -0.52734375 to 0.52734375
- step_raw: float32 [4, 1536, 128], P('section', 'ctx', 'tp'), may hold values from -6 to 5
- step_bias: float32 [4, 128], P('section', 'tp'), may hold values from -1 to 0.5
- decay_rate: float32 [4, 128], P('section', 'tp'), may hold values from 0.00032552083 to 0.12, as said below
- skip_scale: float32 [4, 128], P('section', 'tp'), may hold values from 0.5 to 2
- norm_gain: float32 [4, 8192], P('section', 'tp'), may hold values from 0.1 to 1.9
- out_weight: bfloat16 [4, 8192, 4096], P('section', 'tp'), may hold values from -0.09375 to 0.09375
- residual: bfloat16 [4, 1536, 4096], P('section', 'ctx', 'tp'), may hold values from -6 to 6
Outputs:
- next_input: bfloat16 [4, 1536, 4096], P('section', 'ctx', 'tp')
The draws below stay inside these ranges and needn't reach their ends.
Inputs may be any that keep to these rules, and one draw needn't show every extreme that they name: `decay_rate`: positive decay rates per head.
All inputs are finite; a program needn't handle non-finite values.
Results may differ from the reference program's by a relative error of at most 0.017.
Values may be sent and summed in bfloat16 or wider, within the bound.
A program may use at most 128 MiB of HBM per device.

```python
import jax
import jax.numpy as jnp
from jax import lax

D = 4096
HEADS = 128
HEAD_DIM = 64
STATE = 128
GROUPS = 8
BLOCK = 128
TOK_DEV = 384
INNER = 8192
TOKENS = 1536
SECTIONS = 4
N_TP = 2


def draw_decay_rate(key, part):
    k_pick, k_slow, k_fast = jax.random.split(jax.random.fold_in(key, 7), 3)
    order = jax.random.permutation(k_pick, SECTIONS * HEADS).reshape(SECTIONS, HEADS)
    share = 0.5
    slow_heads = order.astype(jnp.float32) < share * SECTIONS * HEADS
    slow_rate = jnp.exp(jax.random.uniform(k_slow, (SECTIONS, HEADS), jnp.float32, jnp.log(0.5), jnp.log(2.0))) / TOKENS
    fast_rate = jnp.exp(jax.random.uniform(k_fast, (SECTIONS, HEADS), jnp.float32, jnp.log(0.03), jnp.log(0.12)))
    return jnp.where(slow_heads, slow_rate, fast_rate).astype(jnp.float32)


def draw_step_raw(key, part):
    k_level, k_head, k_noise = jax.random.split(jax.random.fold_in(key, 11), 3)
    stretches = TOKENS // TOK_DEV
    levels = jax.random.uniform(k_level, (SECTIONS, stretches, 1), jnp.float32, -2.5, 1.5)
    levels = jnp.repeat(levels, TOK_DEV, axis=1)
    jitter = jax.random.uniform(k_head, (SECTIONS, 1, HEADS), jnp.float32, -0.5, 0.5)
    noise = jnp.clip(0.4 * jax.random.normal(k_noise, (SECTIONS, TOKENS, HEADS), jnp.float32), -1.6, 1.6)
    return (levels + jitter + noise).astype(jnp.float32)


def strengthened(drawn, stream_key, source, target, parts, factor):
    owner, partner = [(jnp.arange(drawn.shape[dim]) // (drawn.shape[dim] // parts)).reshape([-1 if axis == dim else 1 for axis in range(drawn.ndim)]) for dim in (source, target)]
    chosen = jax.random.permutation(stream_key, parts)[partner]
    strong = (owner == chosen) | (owner == (partner + parts // 2) % parts)
    return jnp.where(strong, factor * drawn, drawn)


def block_levels(rng, dims, shards, smallest, top_value):
    def one(axis_at, parts):
        heights = jax.random.uniform(jax.random.fold_in(jax.random.fold_in(rng, 6), axis_at), (parts,), jnp.float32, smallest / len(shards), top_value / len(shards))
        return jnp.repeat(jnp.exp(heights), dims[axis_at] // parts).reshape((-1,) + (1,) * (len(dims) - axis_at - 1))

    gain = one(*shards[0])
    for cut in shards[1:]:
        gain = gain * one(*cut)
    return gain


def bell_draw(stream_key, extent, spread, limit, cuts=(), held_as=jnp.bfloat16):
    drawn = spread * jax.random.normal(stream_key, extent, jnp.float32)
    if cuts:
        drawn = drawn * block_levels(stream_key, extent, cuts, -0.22, 0.18)
    return jnp.clip(drawn, -limit, limit).astype(held_as)


def heavy_noise(rng, extent, scale, most, pieces, heavy, kind=jnp.bfloat16):
    values = scale * jax.random.normal(rng, extent, jnp.float32)
    if pieces:
        values = values * block_levels(rng, extent, pieces, -0.22, 0.18)
    return jnp.clip(strengthened(values, jax.random.fold_in(rng, 3), *heavy), -most, most).astype(kind)


def setup_inputs(seed: int = 0) -> dict:
    streams_of = jax.random.split(jax.random.key(seed), 12)
    head_input = bell_draw(streams_of[0], (SECTIONS, TOKENS, INNER), 1.0, 6.0, ((0, 4), (1, 4), (2, 2)))
    gate_input = bell_draw(streams_of[1], (SECTIONS, TOKENS, INNER), 1.0, 6.0, ((0, 4), (1, 4), (2, 2)))
    b_input = bell_draw(streams_of[2], (SECTIONS, TOKENS, GROUPS * STATE), (STATE ** -0.5), 0.52734375, ((0, 4), (1, 4), (2, 2)))
    c_input = bell_draw(streams_of[3], (SECTIONS, TOKENS, GROUPS * STATE), (STATE ** -0.5), 0.52734375, ((0, 4), (1, 4), (2, 2)))
    step_raw = draw_step_raw(jax.random.fold_in(streams_of[11], 71), 0)
    step_bias = jnp.clip(-1.0 + 1.5 * jax.random.uniform(streams_of[5], (SECTIONS, HEADS), jnp.float32) ** block_levels(streams_of[5], (SECTIONS, HEADS), ((0, 4), (1, 2)), -0.2, 0.2), -1.0, 0.5)
    decay_rate = draw_decay_rate(jax.random.fold_in(streams_of[11], 71), 0)
    skip_scale = jnp.clip(0.5 + 1.5 * jax.random.uniform(streams_of[7], (SECTIONS, HEADS), jnp.float32) ** block_levels(streams_of[7], (SECTIONS, HEADS), ((0, 4), (1, 2)), -0.2, 0.2), 0.5, 2.0)
    norm_gain = jnp.clip(1.0 + 0.18 * jax.random.normal(streams_of[8], (SECTIONS, INNER), jnp.float32), 0.1, 1.9)
    out_weight = heavy_noise(streams_of[9], (SECTIONS, INNER, D), INNER ** -0.5, 0.09375, ((0, 4), (1, 2)), (1, 2, 2, 2.0))
    residual = bell_draw(streams_of[10], (SECTIONS, TOKENS, D), 1.0, 6.0, ((0, 4), (1, 4), (2, 2)))
    return dict(head_input=head_input, gate_input=gate_input, b_input=b_input, c_input=c_input, step_raw=step_raw, step_bias=step_bias, decay_rate=decay_rate, skip_scale=skip_scale, norm_gain=norm_gain, out_weight=out_weight, residual=residual)


def scan_mixer(head_input, b_input, c_input, step_raw, step_bias, decay_rate, skip_scale):
    highest = lax.Precision.HIGHEST
    length = head_input.shape[0]
    blocks = length // BLOCK
    repeats = HEADS // GROUPS
    values = head_input.astype(jnp.float32).reshape(blocks, BLOCK, HEADS, HEAD_DIM)
    b_heads = jnp.repeat(b_input.astype(jnp.float32).reshape(blocks, BLOCK, GROUPS, STATE), repeats, axis=2)
    c_heads = jnp.repeat(c_input.astype(jnp.float32).reshape(blocks, BLOCK, GROUPS, STATE), repeats, axis=2)
    steps = jax.nn.softplus(step_raw + step_bias[None, :])
    logdecay = (-decay_rate[None, :] * steps).reshape(blocks, BLOCK, HEADS)
    steps = steps.reshape(blocks, BLOCK, HEADS)
    lower_mask = jnp.tril(jnp.ones((BLOCK, BLOCK), dtype=jnp.bool_))

    def block_step(carried, items):
        x_blk, b_blk, c_blk, step_blk, decay_blk = items
        cumulative = jnp.cumsum(decay_blk, axis=0)
        cum_heads = cumulative.T
        log_gap = cum_heads[:, :, None] - cum_heads[:, None, :]
        decays = jnp.where(lower_mask[None], jnp.exp(jnp.where(lower_mask[None], log_gap, 0.0)), 0.0)
        scores = jnp.einsum('thn,shn->hts', c_blk, b_blk, precision=highest)
        weights = (scores * decays * step_blk.T[:, None, :]).astype(jnp.bfloat16).astype(jnp.float32)
        output = jnp.einsum('hts,shp->thp', weights, x_blk, precision=highest)
        out_map = (c_blk * jnp.exp(cumulative)[:, :, None]).astype(jnp.bfloat16).astype(jnp.float32)
        start_low = carried.astype(jnp.bfloat16).astype(jnp.float32)
        output = output + jnp.einsum('thn,hnp->thp', out_map, start_low, precision=highest)
        end_weight = jnp.exp(cum_heads[:, -1:] - cum_heads) * step_blk.T
        in_map = (end_weight.T[:, :, None] * b_blk).astype(jnp.bfloat16).astype(jnp.float32)
        fresh = jnp.einsum('shn,shp->hnp', in_map, x_blk, precision=highest)
        carried = jnp.exp(cum_heads[:, -1])[:, None, None] * carried + fresh
        return (carried, output)
    start_state = jnp.zeros((HEADS, STATE, HEAD_DIM), jnp.float32)
    _, outputs = lax.scan(block_step, start_state, (values, b_heads, c_heads, steps, logdecay))
    outputs = outputs + skip_scale[None, None, :, None] * values
    return outputs.reshape(length, HEADS * HEAD_DIM)

def reference(head_input, gate_input, b_input, c_input, step_raw, step_bias, decay_rate, skip_scale, norm_gain, out_weight, residual):
    results = []
    width = HEADS * HEAD_DIM
    slice_width = width // N_TP
    for section_index in range(SECTIONS):
        scan_out = scan_mixer(head_input[section_index], b_input[section_index], c_input[section_index], step_raw[section_index], step_bias[section_index], decay_rate[section_index], skip_scale[section_index])
        gated = scan_out * jax.nn.silu(gate_input[section_index].astype(jnp.float32))
        grouped = gated.reshape(gated.shape[0], GROUPS, width // GROUPS)
        mean_square = lax.optimization_barrier(jnp.mean(grouped * grouped, axis=-1, keepdims=True))
        normed = (grouped * lax.rsqrt(mean_square + 1e-05)).reshape(gated.shape[0], width)
        normed = (normed * norm_gain[section_index][None, :]).astype(jnp.bfloat16)
        mixed = jnp.zeros((gated.shape[0], D), jnp.float32)
        for slice_index in range(N_TP):
            lower = slice_index * slice_width
            partial_value = jnp.dot(normed[:, lower:lower + slice_width], out_weight[section_index, lower:lower + slice_width], preferred_element_type=jnp.float32)
            partial_value = lax.optimization_barrier(partial_value.astype(jnp.bfloat16)).astype(jnp.float32)
            mixed = mixed + partial_value
        results.append((residual[section_index].astype(jnp.float32) + mixed).astype(jnp.bfloat16))
    stacked = jnp.stack(results, axis=0)
    return jnp.roll(stacked, 1, axis=0)
```

```python
import functools

import jax
import jax.numpy as jnp
from jax import lax
from jax.experimental import pallas as pl
from jax.experimental.pallas import tpu as pltpu
from jax.sharding import PartitionSpec as P

HEAD_DIM = 64
STATE = 128
BLOCK = 128
CHUNKS = 2
TILE = 256
MESH = pl.DeviceIdType.MESH
F32 = jnp.float32
BF16 = jnp.bfloat16


def parts_of(v, n):
    out = []
    for _ in range(n):
        hi = v.astype(BF16)
        out.append(hi)
        v = v - hi.astype(F32)
    return out


def dot(a, b):
    return jnp.dot(a, b, preferred_element_type=F32)


def lane_spread(v, onehot, n):
    return sum(dot(p, onehot) for p in parts_of(v, n))


def kernel(
    sizes,
    x_hbm,
    gate_hbm,
    b_ref,
    c_ref,
    raw_ref,
    bias_ref,
    rate_ref,
    skip_ref,
    gain_ref,
    w_hbm,
    res_hbm,
    o_ref,
    xv,
    gv,
    wv,
    rv,
    fx,
    fresh,
    total,
    st,
    onehot,
    rows,
    rowx,
    e_ref,
    f_ref,
    pin,
    pout,
    gbuf,
    nbuf,
    acc,
    sbuf,
    rbuf,
    fbuf,
    x_sem,
    g_sem,
    w_sem,
    r_sem,
    ps_sem,
    pr_sem,
    ts_sem,
    tr_sem,
    ss_sem,
    sr_sem,
):
    n_sec, n_ctx, n_tp = sizes
    length, width = x_hbm.shape
    model = w_hbm.shape[1]
    heads = raw_ref.shape[1]
    groups = b_ref.shape[1] // STATE
    gw = width // groups
    per_group = heads // groups
    blocks = length // BLOCK
    cw = gw // CHUNKS
    share = model // n_tp
    tiles = share // TILE
    sec = lax.axis_index("section")
    ctx = lax.axis_index("ctx")
    tp = lax.axis_index("tp")
    sec_next = lax.rem(sec + 1, n_sec)
    sec_prev = lax.rem(sec + n_sec - 1, n_sec)
    ctx_next = lax.rem(ctx + 1, n_ctx)
    ctx_prev = lax.rem(ctx + n_ctx - 1, n_ctx)
    first = ctx == 0
    has_next = ctx < n_ctx - 1

    def gcols(g):
        return pl.ds(pl.multiple_of(g * gw, gw), gw)

    def ccols(g, j):
        return pl.ds(pl.multiple_of(g * gw + j * cw, cw), cw)

    def krows(k):
        return pl.ds(k * BLOCK, BLOCK)

    def x_copy(g):
        return pltpu.make_async_copy(x_hbm.at[:, gcols(g)], xv.at[:, gcols(g)], x_sem.at[g])

    def w_copy(g):
        slot = lax.rem(g, 2)
        return pltpu.make_async_copy(
            w_hbm.at[pl.ds(pl.multiple_of(g * gw, gw), gw), :], wv.at[slot], w_sem.at[slot]
        )

    g_copy = pltpu.make_async_copy(gate_hbm, gv, g_sem)
    r_copy = pltpu.make_async_copy(res_hbm, rv, r_sem)

    barrier = pltpu.get_barrier_semaphore()
    greet = [{"ctx": ctx_next}, {"ctx": ctx_prev}, {"section": sec_next}, {"section": sec_prev}]
    greet += [{"tp": lax.rem(tp + o, n_tp)} for o in range(1, n_tp)]
    for who in greet:
        pl.semaphore_signal(barrier, inc=1, device_id=who, device_id_type=MESH)
    for g in range(groups):
        x_copy(g).start()
    g_copy.start()
    for g in range(min(2, groups)):
        w_copy(g).start()
    r_copy.start()

    at_row = lax.broadcasted_iota(jnp.int32, (BLOCK, BLOCK), 0)
    at_col = lax.broadcasted_iota(jnp.int32, (BLOCK, BLOCK), 1)
    lower = at_row >= at_col
    lower_one = jnp.where(lower, 1.0, 0.0).astype(BF16)
    rows[...] = jnp.zeros_like(rows)
    for k in range(blocks):
        v = raw_ref[krows(k), :] + bias_ref[...]
        step = jnp.maximum(v, 0.0) + jnp.log1p(jnp.exp(-jnp.abs(v)))
        decay = -rate_ref[...] * step
        cum = sum(dot(lower_one, p) for p in parts_of(decay, 3))
        mid = 0.5 * cum[BLOCK - 1 :, :]
        e_ref[krows(k), :] = jnp.exp(cum - mid)
        f_ref[krows(k), :] = step * jnp.exp(mid - cum)
        rows[k : k + 1, :] = jnp.exp(mid)
    rows[blocks : blocks + 1, :] = skip_ref[...]

    pl.semaphore_wait(barrier, len(greet))

    def p_copy(g, j):
        q = g * CHUNKS + j
        return pltpu.make_async_remote_copy(
            src_ref=pout.at[q],
            dst_ref=pin.at[q],
            send_sem=ps_sem.at[q],
            recv_sem=pr_sem.at[q],
            device_id={"ctx": ctx_next},
            device_id_type=MESH,
        )

    @pl.loop(0, groups)
    def _(g):
        head = lax.broadcasted_iota(jnp.int32, (heads, gw), 0)
        lane = lax.broadcasted_iota(jnp.int32, (heads, gw), 1)
        start = (head - g * per_group) * HEAD_DIM
        one = jnp.where((lane >= start) & (lane < start + HEAD_DIM), 1.0, 0.0).astype(BF16)
        onehot[:, gcols(g)] = one
        rowx[:, gcols(g)] = lane_spread(rows[...], one, 3)
        x_copy(g).wait()
        for j in range(CHUNKS):
            cols = ccols(g, j)
            for k in range(blocks):
                scale = lane_spread(f_ref[krows(k), :], onehot[:, cols], 2)
                scaled = (scale * xv[krows(k), cols].astype(F32)).astype(BF16)
                fx[krows(k), cols] = scaled
                b_blk = b_ref[krows(k), pl.ds(pl.multiple_of(g * STATE, STATE), STATE)]
                new = lax.dot_general(
                    b_blk, scaled, (((0,), (0,)), ((), ())), preferred_element_type=F32
                )
                q = rowx[k : k + 1, cols]
                new = new * q
                fresh[k, :, cols] = new
                if k == 0:
                    total[:, cols] = new
                else:
                    total[:, cols] = total[:, cols] * (q * q) + new

            @pl.when(first)
            def _():
                pin[g * CHUNKS + j] = jnp.zeros((STATE, cw), BF16)
                pout[g * CHUNKS + j] = total[:, cols].astype(BF16)
                p_copy(g, j).start()

    g_copy.wait()

    @pl.loop(0, length // BLOCK)
    def _(k):
        acc[pl.ds(pl.multiple_of(k * BLOCK, BLOCK), BLOCK), :] = jnp.zeros((BLOCK, model), F32)

    @pl.loop(0, groups)
    def _(g):
        for j in range(CHUNKS):
            cols = ccols(g, j)
            q = g * CHUNKS + j

            @pl.when(jnp.logical_not(first))
            def _():
                p_copy(g, j).wait_recv()

                @pl.when(has_next)
                def _():
                    whole = rowx[0:1, cols]
                    for k in range(1, blocks):
                        whole = whole * rowx[k : k + 1, cols]
                    out = total[:, cols] + pin[q].astype(F32) * (whole * whole)
                    pout[q] = out.astype(BF16)
                    p_copy(g, j).start()

            st[:, j * cw : (j + 1) * cw] = pin[q].astype(F32)

        for k in range(blocks):
            state_cols = pl.ds(pl.multiple_of(g * STATE, STATE), STATE)
            b_blk = b_ref[krows(k), state_cols]
            c_blk = c_ref[krows(k), state_cols]
            cb = lax.dot_general(
                c_blk, b_blk, (((1,), (1,)), ((), ())), preferred_element_type=F32
            )
            left = jnp.concatenate([jnp.where(lower, cb, 0.0).astype(BF16), c_blk], axis=1)
            squares = jnp.zeros((BLOCK, 1), F32)
            for j in range(CHUNKS):
                cols = ccols(g, j)
                here = slice(j * cw, (j + 1) * cw)
                q = rowx[k : k + 1, cols]
                state = st[:, here]
                right = jnp.concatenate([fx[krows(k), cols], (state * q).astype(BF16)], axis=0)
                y = dot(left, right) * lane_spread(e_ref[krows(k), :], onehot[:, cols], 2)
                y = y + rowx[blocks : blocks + 1, cols] * xv[krows(k), cols].astype(F32)
                gate = gv[krows(k), cols].astype(F32)
                y = y * (gate / (1.0 + jnp.exp(-gate)))
                gbuf[:, here] = y
                squares = squares + jnp.sum(y * y, axis=1, keepdims=True)
                if k < blocks - 1:
                    st[:, here] = state * (q * q) + fresh[k, :, cols]
            norm = lax.rsqrt(squares * (1.0 / gw) + 1e-05)
            nbuf[krows(k), :] = (gbuf[...] * norm * gain_ref[:, gcols(g)]).astype(BF16)

        w_copy(g).wait()

        @pl.when(g < groups - 1)
        def _():
            slot = lax.rem(g, 2)

            @pl.loop(0, model // TILE)
            def _(t):
                at = pl.ds(pl.multiple_of(t * TILE, TILE), TILE)
                acc[:, at] += dot(nbuf[...], wv[slot, :, at])

            @pl.when(g + 2 < groups)
            def _():
                w_copy(g + 2).start()

    last = (groups - 1) % 2

    def finished(at):
        return (acc[:, at] + dot(nbuf[...], wv[last, :, at])).astype(BF16)

    def t_copy(o, t):
        return pltpu.make_async_remote_copy(
            src_ref=sbuf.at[o - 1, t],
            dst_ref=rbuf.at[o - 1, t],
            send_sem=ts_sem.at[o - 1, t],
            recv_sem=tr_sem.at[o - 1, t],
            device_id={"tp": lax.rem(tp + o, n_tp)},
            device_id_type=MESH,
        )

    def s_copy(t):
        return pltpu.make_async_remote_copy(
            src_ref=fbuf.at[t],
            dst_ref=o_ref.at[:, pl.ds(pl.multiple_of(t * TILE, TILE), TILE)],
            send_sem=ss_sem.at[t],
            recv_sem=sr_sem.at[t],
            device_id={"section": sec_next},
            device_id_type=MESH,
        )

    @pl.loop(0, tiles)
    def _(t):
        for o in range(1, n_tp):
            peer = lax.rem(tp + o, n_tp)
            at = pl.ds(pl.multiple_of(peer * share + t * TILE, TILE), TILE)
            sbuf[o - 1, t] = finished(at)
            t_copy(o, t).start()

    r_copy.wait()

    @pl.loop(0, tiles)
    def _(t):
        at = pl.ds(pl.multiple_of(tp * share + t * TILE, TILE), TILE)
        here = pl.ds(pl.multiple_of(t * TILE, TILE), TILE)
        acc[:, at] = finished(at).astype(F32) + rv[:, here].astype(F32)

    @pl.loop(0, tiles)
    def _(t):
        at = pl.ds(pl.multiple_of(tp * share + t * TILE, TILE), TILE)
        mixed = acc[:, at]
        for o in range(1, n_tp):
            t_copy(o, t).wait_recv()
            mixed = mixed + rbuf[o - 1, t].astype(F32)
        fbuf[t] = mixed.astype(BF16)
        s_copy(t).start()

    @pl.when(has_next)
    def _():
        @pl.loop(0, groups)
        def _(g):
            for j in range(CHUNKS):
                p_copy(g, j).wait_send()

    @pl.loop(0, tiles)
    def _(t):
        for o in range(1, n_tp):
            t_copy(o, t).wait_send()
        s_copy(t).wait()


def on_device(
    sizes,
    head_input,
    gate_input,
    b_input,
    c_input,
    step_raw,
    step_bias,
    decay_rate,
    skip_scale,
    norm_gain,
    out_weight,
    residual,
):
    n_sec, n_ctx, n_tp = sizes
    length, width = head_input.shape[1:]
    model = out_weight.shape[2]
    heads = step_raw.shape[2]
    groups = b_input.shape[2] // STATE
    gw = width // groups
    blocks = length // BLOCK
    share = model // n_tp
    tiles = share // TILE
    row_count = (blocks + 1 + 7) // 8 * 8
    chunks = groups * CHUNKS
    dma = pltpu.SemaphoreType.DMA
    vmem = pl.BlockSpec(memory_space=pltpu.VMEM)
    anywhere = pl.BlockSpec(memory_space=pl.ANY)
    out = pl.pallas_call(
        functools.partial(kernel, sizes),
        out_shape=jax.ShapeDtypeStruct((length, share), BF16),
        in_specs=[anywhere, anywhere] + [vmem] * 7 + [anywhere, anywhere],
        out_specs=anywhere,
        scratch_shapes=[
            pltpu.VMEM((length, width), BF16),
            pltpu.VMEM((length, width), BF16),
            pltpu.VMEM((2, gw, model), BF16),
            pltpu.VMEM((length, share), BF16),
            pltpu.VMEM((length, width), BF16),
            pltpu.VMEM((blocks, STATE, width), F32),
            pltpu.VMEM((STATE, width), F32),
            pltpu.VMEM((STATE, gw), F32),
            pltpu.VMEM((heads, width), BF16),
            pltpu.VMEM((row_count, heads), F32),
            pltpu.VMEM((row_count, width), F32),
            pltpu.VMEM((length, heads), F32),
            pltpu.VMEM((length, heads), F32),
            pltpu.VMEM((chunks, STATE, gw // CHUNKS), BF16),
            pltpu.VMEM((chunks, STATE, gw // CHUNKS), BF16),
            pltpu.VMEM((BLOCK, gw), F32),
            pltpu.VMEM((length, gw), BF16),
            pltpu.VMEM((length, model), F32),
            pltpu.VMEM((n_tp - 1, tiles, length, TILE), BF16),
            pltpu.VMEM((n_tp - 1, tiles, length, TILE), BF16),
            pltpu.VMEM((tiles, length, TILE), BF16),
            dma((groups,)),
            dma,
            dma((2,)),
            dma,
            dma((chunks,)),
            dma((chunks,)),
            dma((n_tp - 1, tiles)),
            dma((n_tp - 1, tiles)),
            dma((tiles,)),
            dma((tiles,)),
        ],
        compiler_params=pltpu.CompilerParams(
            collective_id=0, has_side_effects=True, vmem_limit_bytes=63 * 1024 * 1024
        ),
    )(
        head_input[0],
        gate_input[0],
        b_input[0],
        c_input[0],
        step_raw[0],
        step_bias,
        decay_rate,
        skip_scale,
        norm_gain,
        out_weight[0],
        residual[0],
    )
    return out[None]


def solution(mesh):
    sizes = tuple(mesh.shape[name] for name in ("section", "ctx", "tp"))
    whole = P("section", "ctx", "tp")
    heads = P("section", "tp")
    placed = (whole,) * 5 + (heads,) * 4 + (P("section", "tp", None), whole)
    return jax.shard_map(
        functools.partial(on_device, sizes),
        mesh=mesh,
        in_specs=placed,
        out_specs=whole,
        check_vma=False,
    )
```

```python
import functools

import jax
import jax.numpy as jnp
from jax import lax
from jax.experimental import pallas as pl
from jax.experimental.pallas import tpu as pltpu
from jax.sharding import PartitionSpec as P

HEAD_DIM = 64
STATE = 128
BLOCK = 128
CHUNKS = 2
TILE = 256
MESH = pl.DeviceIdType.MESH
F32 = jnp.float32
BF16 = jnp.bfloat16


def parts_of(v, n):
    out = []
    for _ in range(n):
        hi = v.astype(BF16)
        out.append(hi)
        v = v - hi.astype(F32)
    return out


def dot(a, b):
    return jnp.dot(a, b, preferred_element_type=F32)


def halves(v):
    return jnp.concatenate(parts_of(v, 2), axis=1)


def kernel(
    sizes,
    x_hbm,
    gate_hbm,
    b_ref,
    c_ref,
    raw_ref,
    bias_ref,
    rate_ref,
    skip_ref,
    gain_ref,
    w_hbm,
    res_hbm,
    o_ref,
    xv,
    gv,
    wv,
    rv,
    fx,
    fresh,
    total,
    left,
    onehot,
    rows,
    rowx,
    e_ref,
    f_ref,
    pin,
    pout,
    gbuf,
    sbuf,
    rbuf,
    fbuf,
    x_sem,
    g_sem,
    w_sem,
    r_sem,
    ps_sem,
    pr_sem,
    ts_sem,
    tr_sem,
    ss_sem,
    sr_sem,
):
    n_sec, n_ctx, n_tp = sizes
    length, width = x_hbm.shape
    model = w_hbm.shape[1]
    heads = raw_ref.shape[0]
    groups = b_ref.shape[1] // STATE
    gw = width // groups
    per_group = heads // groups
    blocks = length // BLOCK
    cw = gw // CHUNKS
    share = model // n_tp
    tiles = share // TILE
    sec = lax.axis_index("section")
    ctx = lax.axis_index("ctx")
    tp = lax.axis_index("tp")
    sec_next = lax.rem(sec + 1, n_sec)
    sec_prev = lax.rem(sec + n_sec - 1, n_sec)
    ctx_next = lax.rem(ctx + 1, n_ctx)
    ctx_prev = lax.rem(ctx + n_ctx - 1, n_ctx)
    first = ctx == 0
    has_next = ctx < n_ctx - 1

    def gcols(g):
        return pl.ds(pl.multiple_of(g * gw, gw), gw)

    def ccols(g, j):
        return pl.ds(pl.multiple_of(g * gw + j * cw, cw), cw)

    def krows(k):
        return pl.ds(k * BLOCK, BLOCK)

    def x_copy(g):
        return pltpu.make_async_copy(x_hbm.at[:, gcols(g)], xv.at[:, gcols(g)], x_sem.at[g])

    def w_copy(o):
        at = pl.ds(pl.multiple_of(lax.rem(tp + o, n_tp) * share, share), share)
        return pltpu.make_async_copy(w_hbm.at[:, at], wv.at[:, at], w_sem.at[o])

    g_copy = pltpu.make_async_copy(gate_hbm, gv, g_sem)
    r_copy = pltpu.make_async_copy(res_hbm, rv, r_sem)

    barrier = pltpu.get_barrier_semaphore()
    greet = [{"ctx": ctx_next}, {"ctx": ctx_prev}, {"section": sec_next}, {"section": sec_prev}]
    greet += [{"tp": lax.rem(tp + o, n_tp)} for o in range(1, n_tp)]
    for who in greet:
        pl.semaphore_signal(barrier, inc=1, device_id=who, device_id_type=MESH)
    for g in range(groups):
        x_copy(g).start()
    g_copy.start()
    for o in range(n_tp):
        w_copy((o + 1) % n_tp).start()
    r_copy.start()

    at_row = lax.broadcasted_iota(jnp.int32, (BLOCK, BLOCK), 0)
    at_col = lax.broadcasted_iota(jnp.int32, (BLOCK, BLOCK), 1)
    lower = at_row >= at_col
    lower_one = jnp.where(lower, 1.0, 0.0).astype(BF16)
    rows[...] = jnp.zeros_like(rows)
    for k in range(blocks):
        v = raw_ref[:, krows(k)].T + bias_ref[...]
        step = jnp.maximum(v, 0.0) + jnp.log1p(jnp.exp(-jnp.abs(v)))
        decay = -rate_ref[...] * step
        cum = sum(dot(lower_one, p) for p in parts_of(decay, 3))
        mid = 0.5 * cum[BLOCK - 1 :, :]
        e_ref[krows(k), :] = halves(jnp.exp(cum - mid))
        f_ref[krows(k), :] = halves(step * jnp.exp(mid - cum))
        rows[k : k + 1, :] = jnp.exp(mid)
    rows[blocks : blocks + 1, :] = skip_ref[...]

    pl.semaphore_wait(barrier, len(greet))

    def p_copy(g, j):
        q = g * CHUNKS + j
        return pltpu.make_async_remote_copy(
            src_ref=pout.at[q],
            dst_ref=pin.at[q],
            send_sem=ps_sem.at[q],
            recv_sem=pr_sem.at[q],
            device_id={"ctx": ctx_next},
            device_id_type=MESH,
        )

    @pl.loop(0, groups)
    def _(g):
        head = lax.broadcasted_iota(jnp.int32, (heads, gw), 0)
        lane = lax.broadcasted_iota(jnp.int32, (heads, gw), 1)
        start = (head - g * per_group) * HEAD_DIM
        one = jnp.where((lane >= start) & (lane < start + HEAD_DIM), 1.0, 0.0).astype(BF16)
        one = jnp.concatenate([one, one], axis=0)
        onehot[:, gcols(g)] = one
        rowx[:, gcols(g)] = dot(halves(rows[...]), one)
        x_copy(g).wait()
        for j in range(CHUNKS):
            cols = ccols(g, j)
            scale = dot(f_ref[...], onehot[:, cols])
            fx[:, cols] = (scale * xv[:, cols].astype(F32)).astype(BF16)
            for k in range(blocks):
                b_blk = b_ref[krows(k), pl.ds(pl.multiple_of(g * STATE, STATE), STATE)]
                new = lax.dot_general(
                    b_blk, fx[krows(k), cols], (((0,), (0,)), ((), ())), preferred_element_type=F32
                )
                q = rowx[k : k + 1, cols]
                new = new * q
                if k < blocks - 1:
                    fresh[k, :, cols] = new
                if k == 0:
                    total[:, cols] = new
                else:
                    total[:, cols] = total[:, cols] * (q * q) + new

            @pl.when(first)
            def _():
                pin[g * CHUNKS + j] = jnp.zeros((STATE, cw), BF16)
                pout[g * CHUNKS + j] = total[:, cols].astype(BF16)
                p_copy(g, j).start()

    @pl.loop(0, groups)
    def _(g):
        state_cols = pl.ds(pl.multiple_of(g * STATE, STATE), STATE)
        for k in range(blocks):
            c_blk = c_ref[krows(k), state_cols]
            cb = lax.dot_general(
                c_blk,
                b_ref[krows(k), state_cols],
                (((1,), (1,)), ((), ())),
                preferred_element_type=F32,
            )
            left[g, krows(k), :STATE] = jnp.where(lower, cb, 0.0).astype(BF16)
            left[g, krows(k), STATE:] = c_blk

    g_copy.wait()

    @pl.loop(0, groups)
    def _(g):
        squares = [jnp.zeros((BLOCK, 1), F32) for _ in range(blocks)]
        for j in range(CHUNKS):
            cols = ccols(g, j)
            here = slice(j * cw, (j + 1) * cw)
            chunk = g * CHUNKS + j

            @pl.when(jnp.logical_not(first))
            def _():
                p_copy(g, j).wait_recv()

                @pl.when(has_next)
                def _():
                    whole = rowx[0:1, cols]
                    for k in range(1, blocks):
                        whole = whole * rowx[k : k + 1, cols]
                    out = total[:, cols] + pin[chunk].astype(F32) * (whole * whole)
                    pout[chunk] = out.astype(BF16)
                    p_copy(g, j).start()

            state = pin[chunk].astype(F32)
            spread = dot(e_ref[...], onehot[:, cols])
            for k in range(blocks):
                q = rowx[k : k + 1, cols]
                right = jnp.concatenate([fx[krows(k), cols], (state * q).astype(BF16)], axis=0)
                y = dot(left[g, krows(k), :], right) * spread[k * BLOCK : (k + 1) * BLOCK]
                y = y + rowx[blocks : blocks + 1, cols] * xv[krows(k), cols].astype(F32)
                half = 0.5 * gv[krows(k), cols].astype(F32)
                y = y * (half + half * jnp.tanh(half))
                gbuf[krows(k), here] = y
                squares[k] = squares[k] + jnp.sum(y * y, axis=1, keepdims=True)
                if k < blocks - 1:
                    state = state * (q * q) + fresh[k, :, cols]
        for k in range(blocks):
            norm = lax.rsqrt(squares[k] * (1.0 / gw) + 1e-05)
            gv[krows(k), gcols(g)] = (gbuf[krows(k), :] * norm * gain_ref[:, gcols(g)]).astype(BF16)

    def finished(at):
        return dot(gv[...], wv[:, at]).astype(BF16)

    def t_copy(o, t):
        return pltpu.make_async_remote_copy(
            src_ref=sbuf.at[o - 1, t],
            dst_ref=rbuf.at[o - 1, t],
            send_sem=ts_sem.at[o - 1, t],
            recv_sem=tr_sem.at[o - 1, t],
            device_id={"tp": lax.rem(tp + o, n_tp)},
            device_id_type=MESH,
        )

    def s_copy(t):
        return pltpu.make_async_remote_copy(
            src_ref=fbuf.at[t],
            dst_ref=o_ref.at[:, pl.ds(pl.multiple_of(t * TILE, TILE), TILE)],
            send_sem=ss_sem.at[t],
            recv_sem=sr_sem.at[t],
            device_id={"section": sec_next},
            device_id_type=MESH,
        )

    for o in range(1, n_tp):
        w_copy(o).wait()

    @pl.loop(0, tiles)
    def _(t):
        for o in range(1, n_tp):
            peer = lax.rem(tp + o, n_tp)
            at = pl.ds(pl.multiple_of(peer * share + t * TILE, TILE), TILE)
            sbuf[o - 1, t] = finished(at)
            t_copy(o, t).start()

    w_copy(0).wait()
    r_copy.wait()

    @pl.loop(0, tiles)
    def _(t):
        at = pl.ds(pl.multiple_of(tp * share + t * TILE, TILE), TILE)
        here = pl.ds(pl.multiple_of(t * TILE, TILE), TILE)
        fbuf[t] = finished(at)
        for o in range(1, n_tp):
            t_copy(o, t).wait_recv()
        mixed = rv[:, here].astype(F32) + fbuf[t].astype(F32)
        for o in range(1, n_tp):
            mixed = mixed + rbuf[o - 1, t].astype(F32)
        fbuf[t] = mixed.astype(BF16)
        s_copy(t).start()

    @pl.when(has_next)
    def _():
        @pl.loop(0, groups)
        def _(g):
            for j in range(CHUNKS):
                p_copy(g, j).wait_send()

    @pl.loop(0, tiles)
    def _(t):
        for o in range(1, n_tp):
            t_copy(o, t).wait_send()
        s_copy(t).wait()


def on_device(
    sizes,
    head_input,
    gate_input,
    b_input,
    c_input,
    step_raw,
    step_bias,
    decay_rate,
    skip_scale,
    norm_gain,
    out_weight,
    residual,
):
    n_sec, n_ctx, n_tp = sizes
    length, width = head_input.shape[1:]
    model = out_weight.shape[2]
    heads = step_raw.shape[2]
    groups = b_input.shape[2] // STATE
    gw = width // groups
    blocks = length // BLOCK
    share = model // n_tp
    tiles = share // TILE
    row_count = (blocks + 1 + 7) // 8 * 8
    chunks = groups * CHUNKS
    dma = pltpu.SemaphoreType.DMA
    vmem = pl.BlockSpec(memory_space=pltpu.VMEM)
    anywhere = pl.BlockSpec(memory_space=pl.ANY)
    out = pl.pallas_call(
        functools.partial(kernel, sizes),
        out_shape=jax.ShapeDtypeStruct((length, share), BF16),
        in_specs=[anywhere, anywhere] + [vmem] * 7 + [anywhere, anywhere],
        out_specs=anywhere,
        scratch_shapes=[
            pltpu.VMEM((length, width), BF16),
            pltpu.VMEM((length, width), BF16),
            pltpu.VMEM((width, model), BF16),
            pltpu.VMEM((length, share), BF16),
            pltpu.VMEM((length, width), BF16),
            pltpu.VMEM((max(blocks - 1, 1), STATE, width), F32),
            pltpu.VMEM((STATE, width), F32),
            pltpu.VMEM((groups, length, 2 * STATE), BF16),
            pltpu.VMEM((2 * heads, width), BF16),
            pltpu.VMEM((row_count, heads), F32),
            pltpu.VMEM((row_count, width), F32),
            pltpu.VMEM((length, 2 * heads), BF16),
            pltpu.VMEM((length, 2 * heads), BF16),
            pltpu.VMEM((chunks, STATE, gw // CHUNKS), BF16),
            pltpu.VMEM((chunks, STATE, gw // CHUNKS), BF16),
            pltpu.VMEM((length, gw), F32),
            pltpu.VMEM((n_tp - 1, tiles, length, TILE), BF16),
            pltpu.VMEM((n_tp - 1, tiles, length, TILE), BF16),
            pltpu.VMEM((tiles, length, TILE), BF16),
            dma((groups,)),
            dma,
            dma((n_tp,)),
            dma,
            dma((chunks,)),
            dma((chunks,)),
            dma((n_tp - 1, tiles)),
            dma((n_tp - 1, tiles)),
            dma((tiles,)),
            dma((tiles,)),
        ],
        compiler_params=pltpu.CompilerParams(
            collective_id=0, has_side_effects=True, vmem_limit_bytes=67043328
        ),
    )(
        head_input[0],
        gate_input[0],
        b_input[0],
        c_input[0],
        step_raw[0].T,
        step_bias,
        decay_rate,
        skip_scale,
        norm_gain,
        out_weight[0],
        residual[0],
    )
    return out[None]


def solution(mesh):
    sizes = tuple(mesh.shape[name] for name in ("section", "ctx", "tp"))
    whole = P("section", "ctx", "tp")
    heads = P("section", "tp")
    placed = (whole,) * 5 + (heads,) * 4 + (P("section", "tp", None), whole)
    return jax.shard_map(
        functools.partial(on_device, sizes),
        mesh=mesh,
        in_specs=placed,
        out_specs=whole,
        check_vma=False,
    )
```
